32 devices in a mesh: row: 16 (over z, y, x), col: 2 (over core).
Axes of the slice: x: 2, y: 2, z: 4, core: 2. Of those that a mesh axis runs over, the one named last changes fastest.
Arguments:
- lanczos_now: float32 [1, 256, 1024], P(None, 'row', 'col'), may hold values from -80 to 80, as said below
- lanczos_prev: float32 [1, 256, 1024], P(None, 'row', 'col'), may hold values from -6 to 6
- beta_prev: float32 [1], replicated, may hold values from 0.3 to 1.5
- valence_energy: float32 [256], P('row'), may hold values from -1.5 to -0.5
- conduction_energy: float32 [1024], P('col'), may hold values from 0.5 to 2.5
- valence_panel: float32 [16384, 256], P(('row', 'col')), may hold values from -0.375 to 0.375
- conduction_panel: float32 [16384, 1024], P(('row', 'col')), may hold values from -0.1875 to 0.1875
- screened_coulomb: float32 [16384, 16384], P('row', 'col'), may hold values from -0.046875 to 0.046875
- bare_coulomb: float32 [16384, 16384], P('row', 'col'), may hold values from -0.046875 to 0.046875
Outputs:
- lanczos_next: float32 [1, 256, 1024], P(None, 'row', 'col')
- coefficients: float32 [1, 2], replicated
The draws below stay inside these ranges and needn't reach their ends.
Inputs may be any that keep to these rules, and one draw needn't show every extreme that they name: `lanczos_now`: real entries; the vectors of a chain are not normalized.
All inputs are finite; a program needn't handle non-finite values.
Results may differ from the reference program's by a relative error of at most 0.0002.
Values sent between devices are 32-bit elements; how exact they have to be, the bound alone decides.
A program may use at most 192 MiB of HBM per device.

```python
import math
import jax
import jax.numpy as jnp
from jax import lax

V = 256
C = 1024
NP = 16384
NVEC = 1


def draw_lanczos_now(key, part):
    noise_key, column_key = jax.random.split(key, 2)
    base = jnp.clip(jax.random.normal(noise_key, (NVEC, V, C), jnp.float32), -6.0, 6.0)
    position = jnp.arange(V, dtype=jnp.float32) / (V - 1)
    row_scale = 10.0 ** (position - 0.5)
    column_scale = jnp.exp(jax.random.uniform(column_key, (C,), jnp.float32, 0.0, math.log(3.0)))
    return base * row_scale[None, :, None] * column_scale[None, None, :]


def block_levels(key, dims, pieces, low, top_value):
    def one(axis_at, parts):
        steps = jax.random.uniform(jax.random.fold_in(jax.random.fold_in(key, 6), axis_at), (parts,), jnp.float32, low / len(pieces), top_value / len(pieces))
        return jnp.repeat(jnp.exp(steps), dims[axis_at] // parts).reshape((-1,) + (1,) * (len(dims) - axis_at - 1))

    factor_of = one(*pieces[0])
    for cut in pieces[1:]:
        factor_of = factor_of * one(*cut)
    return factor_of


def normal_values(stream_key, extent, width, limit, shards=(), kind=jnp.bfloat16):
    loudness = block_levels(stream_key, extent, shards, -0.22, 0.18) if shards else 1.0
    entries = jax.random.normal(stream_key, extent, jnp.float32) * width * loudness
    return jnp.minimum(jnp.maximum(entries, -limit), limit).astype(kind)


def setup_inputs(seed: int = 0) -> dict:
    key_of = jax.random.split(jax.random.key(seed), 10)
    return {
        "lanczos_now": draw_lanczos_now(jax.random.fold_in(key_of[9], 71), 0),
        "lanczos_prev": normal_values(key_of[1], (NVEC, V, C), 1.0, 6.0, ((1, 16), (2, 2)), jnp.float32),
        "beta_prev": jnp.clip(jnp.exp(jax.random.uniform(key_of[2], (NVEC,), jnp.float32, math.log(0.3), math.log(1.5))), 0.3, 1.5),
        "valence_energy": jnp.clip(-1.5 + 1.0 * jax.random.uniform(key_of[3], (V,), jnp.float32) ** block_levels(key_of[3], (V,), ((0, 16),), -0.2, 0.2), -1.5, -0.5),
        "conduction_energy": jnp.clip(0.5 + 2.0 * jax.random.uniform(key_of[4], (C,), jnp.float32) ** block_levels(key_of[4], (C,), ((0, 2),), -0.2, 0.2), 0.5, 2.5),
        "valence_panel": normal_values(key_of[5], (NP, V), V ** -0.5, 0.375, ((0, 32),), jnp.float32),
        "conduction_panel": normal_values(key_of[6], (NP, C), C ** -0.5, 0.1875, ((0, 32),), jnp.float32),
        "screened_coulomb": normal_values(key_of[7], (NP, NP), NP ** -0.5, 0.046875, ((0, 16), (1, 2)), jnp.float32),
        "bare_coulomb": normal_values(key_of[8], (NP, NP), NP ** -0.5, 0.046875, ((0, 16), (1, 2)), jnp.float32),
    }


precise = lax.Precision.HIGHEST
epsilon = 1e-06

def reference(lanczos_now, lanczos_prev, beta_prev, valence_energy, conduction_energy, valence_panel, conduction_panel, screened_coulomb, bare_coulomb):
    products = jnp.einsum('nv,kvc->knc', valence_panel, lanczos_now, precision=precise)
    density = lax.optimization_barrier(jnp.sum(products * conduction_panel[None], axis=2))
    potential = jnp.einsum('mn,kn->km', bare_coulomb, density, precision=precise)
    weighted = potential[:, :, None] * conduction_panel[None]
    exchange = jnp.einsum('mv,kmc->kvc', valence_panel, weighted, precision=precise)
    pair_amp = jnp.einsum('mc,kvc->kmv', conduction_panel, lanczos_now, precision=precise)
    block_size = min(512, NP)
    block_count = NP // block_size

    def one_block(index, total):
        first_row = (index * block_size).astype(jnp.int32)
        pair_rows = lax.dynamic_slice_in_dim(pair_amp, first_row, block_size, 1)
        kernel_rows = lax.dynamic_slice_in_dim(screened_coulomb, first_row, block_size, 0)
        cond_rows = lax.dynamic_slice_in_dim(conduction_panel, first_row, block_size, 0)
        pair_terms = jnp.einsum('kmv,nv->kmn', pair_rows, valence_panel, precision=precise) * kernel_rows[None]
        screened = jnp.einsum('kmn,nv->kmv', pair_terms, valence_panel, precision=precise)
        return total + jnp.einsum('kmv,mc->kvc', screened, cond_rows, precision=precise)
    direct = lax.fori_loop(0, block_count, one_block, jnp.zeros((NVEC, V, C), jnp.float32))
    gaps = conduction_energy[None, None, :] - valence_energy[None, :, None]
    image = gaps * lanczos_now + 2.0 * exchange - direct
    coef_alpha = lax.optimization_barrier(jnp.mean(lanczos_now * image, axis=(1, 2))) / (lax.optimization_barrier(jnp.mean(lanczos_now * lanczos_now, axis=(1, 2))) + epsilon)
    resid = image - coef_alpha[:, None, None] * lanczos_now - beta_prev[:, None, None] * lanczos_prev
    beta_next = jnp.sqrt(lax.optimization_barrier(jnp.mean(resid * resid, axis=(1, 2))) + epsilon)
    return (resid / beta_next[:, None, None], jnp.stack([coef_alpha, beta_next], axis=1))
```

```python
import functools

import jax
import jax.numpy as jnp
from jax import lax
from jax.experimental import pallas as pl
from jax.experimental.pallas import tpu as pltpu
from jax.sharding import PartitionSpec as P

MESH = pl.DeviceIdType.MESH
F32 = jnp.float32
BF16 = jnp.bfloat16
epsilon = 1e-06
LANES = 128
EXTRA = 8


def split(a):
    high = a.astype(BF16)
    return high, (a - high.astype(F32)).astype(BF16)


def dot3(a, b, dims):
    (ah, al), (bh, bl) = a, b
    one = functools.partial(lax.dot_general, dimension_numbers=(dims, ((), ())), preferred_element_type=F32)
    return one(ah, bh) + (one(ah, bl) + one(al, bh))


def flip(index, mask):
    bit = 0
    while mask >> bit:
        if (mask >> bit) & 1:
            index = index + (1 - 2 * ((index // (1 << bit)) % 2)) * (1 << bit)
        bit += 1
    return index


def remote(src, dst, send, recv, where):
    return pltpu.make_async_remote_copy(
        src_ref=src, dst_ref=dst, send_sem=send, recv_sem=recv, device_id=where, device_id_type=MESH
    )


def loop(low, high, body):
    def step(k, carry):
        body(k)
        return carry

    lax.fori_loop(low, high, step, 0)


def vectors_kernel(nrow, ncol, x_ref, full_ref, local_sem, rs, rr, cs, cr):
    r, c = lax.axis_index("row"), lax.axis_index("col")
    h, w = x_ref.shape

    def row_copy(k):
        return remote(
            x_ref, full_ref.at[c, pl.ds(r * h, h)], rs.at[k], rr.at[k], (lax.rem(r + k, nrow), c)
        )

    def col_copy(k):
        return remote(full_ref.at[c], full_ref.at[c], cs.at[k], cr.at[k], (r, lax.rem(c + k, ncol)))

    def col_arrival(k):
        there = lax.rem(c + ncol - k, ncol)
        return remote(full_ref.at[there], full_ref.at[there], cs.at[k], cr.at[k], (r, there))

    def row_arrival(k):
        there = lax.rem(r + nrow - k, nrow)
        part = full_ref.at[c, pl.ds(there * h, h)]
        return remote(x_ref, part, rs.at[k], rr.at[k], (there, c))

    loop(1, nrow, lambda k: row_copy(k).start())
    own = pltpu.make_async_copy(x_ref, full_ref.at[c, pl.ds(r * h, h)], local_sem)
    own.start()
    own.wait()
    loop(1, nrow, lambda k: row_arrival(k).wait_recv())
    loop(1, ncol, lambda k: col_copy(k).start())
    loop(1, ncol, lambda k: col_arrival(k).wait_recv())
    loop(1, nrow, lambda k: row_copy(k).wait_send())
    loop(1, ncol, lambda k: col_copy(k).wait_send())


def kernel_kernel(
    nrow, ncol, blk, item_ref, pair_ref, w_ref, b_ref, s_ref,
    pan, pairs, ah, al, ph, plo, wbuf, bbuf,
    wsem, bsem, local_sem, chip_send, top_send, send, recv, pair_send, pair_recv,
):
    r, c = lax.axis_index("row"), lax.axis_index("col")
    per = nrow // ncol
    bits = per.bit_length() - 1
    tops = ncol.bit_length() - 1
    top, low = r // per, lax.rem(r, per)
    bands = pair_ref.shape[1]
    points = ncol * blk
    unit = wbuf.shape[3] // blk
    units = ncol // unit
    if bits >= 2:
        base = list(range(bits - 1, 1, -1))
        orders = (base + [0, 1], base + [1, 0])
    else:
        orders = (list(range(bits)),) * 2
    positions = sorted(range(per), key=lambda p: (bin(p).count("1"), p))

    def mask_of(i, position):
        return sum(1 << b for at, b in enumerate(orders[(i // unit) % 2]) if (position >> at) & 1)

    def slot(i, mask):
        return flip(low, mask) * ncol + i

    def fetch(u, step, buffer):
        near = slot(u * unit, mask_of(u * unit, positions[step]))
        at = pl.ds(pl.multiple_of(near * blk, unit * blk), unit * blk)
        return (
            pltpu.make_async_copy(w_ref.at[:, at], wbuf.at[buffer, u], wsem.at[buffer, u]),
            pltpu.make_async_copy(b_ref.at[:, at], bbuf.at[buffer, u], bsem.at[buffer, u]),
        )

    def start_fetch(step):
        for u in range(units):
            for copy in fetch(u, step, step % 2):
                copy.start()

    for j in range(ncol):
        mine = c == j
        here = pan.at[low * ncol + j]

        @pl.when(jnp.logical_and(mine, top == c))
        def _():
            pltpu.make_async_copy(item_ref, here, local_sem).start()

        @pl.when(jnp.logical_and(mine, top != c))
        def _():
            remote(item_ref, here, chip_send, recv.at[j, 0], (r, top)).start()

    def pair_copy(k):
        return remote(
            pair_ref, pairs.at[c], pair_send.at[k], pair_recv.at[k], (r, lax.rem(c + k, ncol))
        )

    def pair_arrival(k):
        there = lax.rem(c + ncol - k, ncol)
        return remote(pair_ref, pairs.at[there], pair_send.at[k], pair_recv.at[k], (r, there))

    loop(1, ncol, lambda k: pair_copy(k).start())
    start_fetch(0)
    if per > 1:
        start_fetch(1)
    s_ref[...] = jnp.zeros_like(s_ref)
    pairs[c] = pair_ref[...]

    def top_copy(i, bit):
        here = pan.at[low * ncol + i]
        return remote(
            here, here, top_send.at[i, bit], recv.at[i, 0], (flip(top, 1 << bit) * per + low, c)
        )

    def differs(bit):
        return lax.rem(top, 2 << bit) == lax.rem(c, 2 << bit)

    def forward_copy(i, mask, stage):
        b = orders[(i // unit) % 2][stage]
        part = pan.at[slot(i, mask)]
        return remote(
            part, part, send.at[i, mask, stage], recv.at[i, mask ^ (1 << b)],
            (flip(r, 1 << b), c),
        )

    def arrival(i, mask):
        part = pan.at[slot(i, mask)]
        return remote(part, part, chip_send, recv.at[i, mask], (r, c))

    def stages(position):
        return range(position.bit_length(), bits)

    for step, position in enumerate(positions):
        for i in range(ncol):
            mask = mask_of(i, position)
            if position == 0:

                @pl.when(jnp.logical_and(c == i, top == c))
                def _():
                    pltpu.make_async_copy(item_ref, pan.at[low * ncol + i], local_sem).wait()

                @pl.when(jnp.logical_not(jnp.logical_and(c == i, top == c)))
                def _():
                    arrival(i, 0).wait_recv()

                for bit in reversed(range(tops)):

                    @pl.when(differs(bit))
                    def _():
                        top_copy(i, bit).start()
            else:
                arrival(i, mask).wait_recv()
            for stage in stages(position):
                forward_copy(i, mask, stage).start()
        if position == 0:
            loop(1, ncol, lambda k: pair_arrival(k).wait_recv())
            for j in range(ncol):
                high, rest = split(pairs[j])
                ah[j * blk : (j + 1) * blk] = high
                al[j * blk : (j + 1) * blk] = rest
        buffer = step % 2
        for i in range(ncol):
            high, rest = split(pan[slot(i, mask_of(i, position)), :blk])
            at = slice((i % unit) * blk, (i % unit + 1) * blk)
            ph[i // unit, at] = high
            plo[i // unit, at] = rest
        for u in range(units):
            for copy in fetch(u, step, buffer):
                copy.wait()
        rows = min(256, points)
        width = min(blk, bands)

        for u in range(units):
            p2 = (ph[u], plo[u])
            lines = [
                pan[slot(i, mask_of(i, position)), blk : blk + EXTRA][j : j + 1, :width]
                for i in range(u * unit, (u + 1) * unit)
                for j in range(blk // width)
            ]

            def body(m):
                at = pl.ds(pl.multiple_of(m * rows, rows), rows)
                terms = dot3((ah[at], al[at]), p2, ((1,), (1,))) * wbuf[buffer, u, at]
                s_ref[at, :bands] += dot3(split(terms), p2, ((1,), (0,)))
                total = jnp.zeros((rows, 1), F32)
                for j, line in enumerate(lines):
                    part = bbuf[buffer, u, at, j * width : (j + 1) * width] * line
                    total = total + jnp.sum(part, axis=1, keepdims=True)
                s_ref[at, bands:] += jnp.broadcast_to(total, (rows, LANES))

            loop(0, points // rows, body)
        if step + 2 < per:
            start_fetch(step + 2)

    loop(1, ncol, lambda k: pair_copy(k).wait_send())

    @pl.when(top != c)
    def _():
        remote(item_ref, pan.at[low * ncol], chip_send, recv.at[0, 0], (r, top)).wait_send()

    for i in range(ncol):
        for bit in range(tops):

            @pl.when(differs(bit))
            def _():
                top_copy(i, bit).wait_send()

        for position in positions:
            for stage in stages(position):
                forward_copy(i, mask_of(i, position), stage).wait_send()


def last_kernel(
    nrow, ncol, size, s_ref, pv_ref, pc_ref, x_ref, prev_ref, gap_ref, beta_ref, out_ref, coef_ref,
    sin, kbuf, kin, rbuf, rin, tile1, tin1, tile2, tin2,
    s_send, s_recv, k_send, k_recv, r_send, r_recv, t1_send, t1_recv, t2_send, t2_recv,
):
    r, c = lax.axis_index("row"), lax.axis_index("col")
    blk, bands = pv_ref.shape
    h, w = x_ref.shape
    everyone = nrow * ncol
    me = r * ncol + c

    def col_peer(k):
        return lax.rem(c + k, ncol)

    def row_peer(k):
        return lax.rem(r + k, nrow)

    def s_copy(k):
        at = pl.ds(pl.multiple_of(col_peer(k) * blk, blk), blk)
        return remote(s_ref.at[at], sin.at[k], s_send.at[k], s_recv.at[k], (r, col_peer(k)))

    def k_copy(k):
        return remote(kbuf.at[col_peer(k)], kin.at[k], k_send.at[k], k_recv.at[k], (r, col_peer(k)))

    def r_copy(k):
        return remote(rbuf.at[row_peer(k)], rin.at[k], r_send.at[k], r_recv.at[k], (row_peer(k), c))

    loop(1, ncol, lambda k: s_copy(k).start())
    own = s_ref[pl.ds(pl.multiple_of(c * blk, blk), blk)]
    for k in range(1, ncol):
        s_copy(k).wait_recv()
        own = own + sin[k]
    terms = 2.0 * pv_ref[...] * own[:, bands : bands + 1] - own[:, :bands]
    turned = split(jnp.transpose(terms))
    for j in range(ncol):
        kbuf[j] = dot3(turned, split(pc_ref[:, j * w : (j + 1) * w]), ((1,), (0,)))
    loop(1, ncol, lambda k: k_copy(k).start())
    part = kbuf[c]
    for k in range(1, ncol):
        k_copy(k).wait_recv()
        part = part + kin[k]
    rbuf[...] = part.reshape(nrow, h, w)
    loop(1, nrow, lambda k: r_copy(k).start())
    x = x_ref[...]
    image = gap_ref[...] * x + rbuf[r]
    for k in range(1, nrow):
        r_copy(k).wait_recv()
        image = image + rin[k]

    def whole(a):
        return jnp.sum(jnp.sum(a, axis=0, keepdims=True), axis=1, keepdims=True)

    def shared(value, tile, tin, sends, recvs):
        def copy(k):
            there = lax.rem(me + k, everyone)
            return remote(tile, tin.at[me], sends.at[k], recvs.at[k], (there // ncol, lax.rem(there, ncol)))

        def arrival(k):
            there = lax.rem(me + everyone - k, everyone)
            return remote(tile, tin.at[there], sends.at[k], recvs.at[k], (there // ncol, lax.rem(there, ncol)))

        tile[...] = value
        tin[me] = value
        loop(1, everyone, lambda k: copy(k).start())
        loop(1, everyone, lambda k: arrival(k).wait_recv())
        loop(1, everyone, lambda k: copy(k).wait_send())
        return jnp.sum(tin[...], axis=0)

    line = lax.broadcasted_iota(jnp.int32, (8, LANES), 0)
    sums = shared(jnp.where(line == 0, whole(x * image), whole(x * x)), tile1, tin1, t1_send, t1_recv)
    alpha = (sums[0:1, 0:1] / size) / (sums[1:2, 0:1] / size + epsilon)
    resid = image - alpha * x - beta_ref[...] * prev_ref[...]
    square = jnp.broadcast_to(whole(resid * resid), (8, LANES))
    beta = jnp.sqrt(shared(square, tile2, tin2, t2_send, t2_recv)[0:1, 0:1] / size + epsilon)
    out_ref[...] = resid / beta
    coef_ref[...] = jnp.where(line == 0, alpha, beta)
    loop(1, ncol, lambda k: s_copy(k).wait_send())
    loop(1, ncol, lambda k: k_copy(k).wait_send())
    loop(1, nrow, lambda k: r_copy(k).wait_send())


VM = pl.BlockSpec(memory_space=pltpu.VMEM)
DMA = pltpu.SemaphoreType.DMA
PARAMS = pltpu.CompilerParams(has_side_effects=True, vmem_limit_bytes=56 * 1024 * 1024)


def per_device(
    nrow, ncol, lanczos_now, lanczos_prev, beta_prev, valence_energy, conduction_energy,
    valence_panel, conduction_panel, screened_coulomb, bare_coulomb,
):
    chains, h, w = lanczos_now.shape
    blk, bands = valence_panel.shape
    conduction = conduction_panel.shape[1]
    points = screened_coulomb.shape[0]
    outs = []
    for chain in range(chains):
        x = lanczos_now[chain]
        full = pl.pallas_call(
            functools.partial(vectors_kernel, nrow, ncol),
            out_shape=jax.ShapeDtypeStruct((ncol, bands, w), F32),
            in_specs=[VM],
            out_specs=VM,
            scratch_shapes=[DMA(()), DMA((nrow,)), DMA((nrow,)), DMA((ncol,)), DMA((ncol,))],
            compiler_params=PARAMS,
        )(x)
        vectors = jnp.transpose(full, (1, 0, 2)).reshape(bands, conduction)
        pair = lax.dot_general(
            conduction_panel, vectors, (((1,), (1,)), ((), ())), precision=lax.Precision.HIGH,
            preferred_element_type=F32,
        )
        density = jnp.sum(pair * valence_panel, axis=1)
        width = min(blk, bands)
        lines = density.reshape(blk // width, width)
        lines = jnp.pad(lines, ((0, EXTRA - blk // width), (0, bands - width)))
        item = jnp.concatenate([valence_panel, lines], axis=0)
        unit = max(1, LANES // blk)
        per = nrow // ncol
        stages = max(1, per.bit_length() - 1)
        tops = max(1, ncol.bit_length() - 1)
        screened = pl.pallas_call(
            functools.partial(kernel_kernel, nrow, ncol, blk),
            out_shape=jax.ShapeDtypeStruct((points, bands + LANES), F32),
            in_specs=[VM, VM, pl.BlockSpec(memory_space=pl.ANY), pl.BlockSpec(memory_space=pl.ANY)],
            out_specs=VM,
            scratch_shapes=[
                pltpu.VMEM((nrow, blk + EXTRA, bands), F32),
                pltpu.VMEM((ncol, blk, bands), F32),
                pltpu.VMEM((points, bands), BF16),
                pltpu.VMEM((points, bands), BF16),
                pltpu.VMEM((ncol // unit, unit * blk, bands), BF16),
                pltpu.VMEM((ncol // unit, unit * blk, bands), BF16),
                pltpu.VMEM((2, ncol // unit, points, unit * blk), F32),
                pltpu.VMEM((2, ncol // unit, points, unit * blk), F32),
                DMA((2, ncol)),
                DMA((2, ncol)),
                DMA(()),
                DMA(()),
                DMA((ncol, tops)),
                DMA((ncol, per, stages)),
                DMA((ncol, per)),
                DMA((ncol,)),
                DMA((ncol,)),
            ],
            compiler_params=PARAMS,
        )(item, pair, screened_coulomb, bare_coulomb)
        gaps = conduction_energy[None, :] - valence_energy[:, None]
        beta = jnp.broadcast_to(beta_prev[chain], (1, w))
        everyone = nrow * ncol
        out, coef = pl.pallas_call(
            functools.partial(last_kernel, nrow, ncol, float(bands * conduction)),
            out_shape=(jax.ShapeDtypeStruct((h, w), F32), jax.ShapeDtypeStruct((8, LANES), F32)),
            in_specs=[VM] * 7,
            out_specs=(VM, VM),
            scratch_shapes=[
                pltpu.VMEM((ncol, blk, bands + LANES), F32),
                pltpu.VMEM((ncol, bands, w), F32),
                pltpu.VMEM((ncol, bands, w), F32),
                pltpu.VMEM((nrow, h, w), F32),
                pltpu.VMEM((nrow, h, w), F32),
                pltpu.VMEM((8, LANES), F32),
                pltpu.VMEM((everyone, 8, LANES), F32),
                pltpu.VMEM((8, LANES), F32),
                pltpu.VMEM((everyone, 8, LANES), F32),
            ]
            + [DMA((n,)) for n in (ncol, ncol, ncol, ncol, nrow, nrow) for _ in range(1)]
            + [DMA((everyone,))] * 4,
            compiler_params=PARAMS,
        )(screened, valence_panel, conduction_panel, x, lanczos_prev[chain], gaps, beta)
        outs.append((out, coef[:2, 0]))
    return jnp.stack([o for o, _ in outs]), jnp.stack([k for _, k in outs])


def solution(mesh):
    placed = (
        P(None, "row", "col"),
        P(None, "row", "col"),
        P(),
        P("row"),
        P("col"),
        P(("row", "col"), None),
        P(("row", "col"), None),
        P("row", "col"),
        P("row", "col"),
    )
    return jax.shard_map(
        functools.partial(per_device, mesh.shape["row"], mesh.shape["col"]),
        mesh=mesh,
        in_specs=placed,
        out_specs=(P(None, "row", "col"), P()),
        check_vma=False,
    )
```

```python
import functools

import jax
import jax.numpy as jnp
from jax import lax
from jax.experimental import pallas as pl
from jax.experimental.pallas import tpu as pltpu
from jax.sharding import PartitionSpec as P

MESH = pl.DeviceIdType.MESH
F32 = jnp.float32
BF16 = jnp.bfloat16
epsilon = 1e-06
LANES = 128
EXTRA = 8


def split(a):
    high = a.astype(BF16)
    return high, (a - high.astype(F32)).astype(BF16)


def dot3(a, b, dims):
    (ah, al), (bh, bl) = a, b
    one = functools.partial(lax.dot_general, dimension_numbers=(dims, ((), ())), preferred_element_type=F32)
    return one(ah, bh) + (one(ah, bl) + one(al, bh))


def flip(index, mask):
    bit = 0
    while mask >> bit:
        if (mask >> bit) & 1:
            index = index + (1 - 2 * ((index // (1 << bit)) % 2)) * (1 << bit)
        bit += 1
    return index


def remote(src, dst, send, recv, where):
    return pltpu.make_async_remote_copy(
        src_ref=src, dst_ref=dst, send_sem=send, recv_sem=recv, device_id=where, device_id_type=MESH
    )


def loop(low, high, body):
    def step(k, carry):
        body(k)
        return carry

    lax.fori_loop(low, high, step, 0)


def vectors_kernel(nrow, ncol, x_ref, full_ref, local_sem, rs, rr, cs, cr):
    r, c = lax.axis_index("row"), lax.axis_index("col")
    h, w = x_ref.shape

    def row_copy(k):
        return remote(
            x_ref, full_ref.at[c, pl.ds(r * h, h)], rs.at[k], rr.at[k], (lax.rem(r + k, nrow), c)
        )

    def col_copy(k):
        return remote(full_ref.at[c], full_ref.at[c], cs.at[k], cr.at[k], (r, lax.rem(c + k, ncol)))

    def col_arrival(k):
        there = lax.rem(c + ncol - k, ncol)
        return remote(full_ref.at[there], full_ref.at[there], cs.at[k], cr.at[k], (r, there))

    def row_arrival(k):
        there = lax.rem(r + nrow - k, nrow)
        part = full_ref.at[c, pl.ds(there * h, h)]
        return remote(x_ref, part, rs.at[k], rr.at[k], (there, c))

    loop(1, nrow, lambda k: row_copy(k).start())
    own = pltpu.make_async_copy(x_ref, full_ref.at[c, pl.ds(r * h, h)], local_sem)
    own.start()
    own.wait()
    loop(1, nrow, lambda k: row_arrival(k).wait_recv())
    loop(1, ncol, lambda k: col_copy(k).start())
    loop(1, ncol, lambda k: col_arrival(k).wait_recv())
    loop(1, nrow, lambda k: row_copy(k).wait_send())
    loop(1, ncol, lambda k: col_copy(k).wait_send())


def kernel_kernel(
    nrow, ncol, blk, item_ref, pair_ref, w_ref, b_ref, s_ref,
    pan, pairs, ah, al, ph, plo, wbuf, bbuf,
    wsem, bsem, local_sem, chip_send, top_send, send, recv, pair_send, pair_recv,
):
    r, c = lax.axis_index("row"), lax.axis_index("col")
    per = nrow // ncol
    bits = per.bit_length() - 1
    tops = ncol.bit_length() - 1
    top, low = r // per, lax.rem(r, per)
    bands = pair_ref.shape[1]
    points = ncol * blk
    unit = wbuf.shape[3] // blk
    units = ncol // unit
    if bits >= 2:
        base = list(range(bits - 1, 1, -1))
        orders = (base + [0, 1], base + [1, 0])
    else:
        orders = (list(range(bits)),) * 2
    positions = sorted(range(per), key=lambda p: (bin(p).count("1"), p))

    def mask_of(i, position):
        return sum(1 << b for at, b in enumerate(orders[(i // unit) % 2]) if (position >> at) & 1)

    def slot(i, mask):
        return flip(low, mask) * ncol + i

    def fetch(u, step, buffer):
        near = slot(u * unit, mask_of(u * unit, positions[step]))
        at = pl.ds(pl.multiple_of(near * blk, unit * blk), unit * blk)
        return (
            pltpu.make_async_copy(w_ref.at[:, at], wbuf.at[buffer, u], wsem.at[buffer, u]),
            pltpu.make_async_copy(b_ref.at[:, at], bbuf.at[buffer, u], bsem.at[buffer, u]),
        )

    def start_fetch(step):
        for u in range(units):
            for copy in fetch(u, step, step % 2):
                copy.start()

    for j in range(ncol):
        mine = c == j
        here = pan.at[low * ncol + j]

        @pl.when(jnp.logical_and(mine, top == c))
        def _():
            pltpu.make_async_copy(item_ref, here, local_sem).start()

        @pl.when(jnp.logical_and(mine, top != c))
        def _():
            remote(item_ref, here, chip_send, recv.at[j, 0], (r, top)).start()

    def pair_copy(k):
        return remote(
            pair_ref, pairs.at[c], pair_send.at[k], pair_recv.at[k], (r, lax.rem(c + k, ncol))
        )

    def pair_arrival(k):
        there = lax.rem(c + ncol - k, ncol)
        return remote(pair_ref, pairs.at[there], pair_send.at[k], pair_recv.at[k], (r, there))

    loop(1, ncol, lambda k: pair_copy(k).start())
    start_fetch(0)
    if per > 1:
        start_fetch(1)
    s_ref[...] = jnp.zeros_like(s_ref)
    pairs[c] = pair_ref[...]

    def top_copy(i, bit):
        here = pan.at[low * ncol + i]
        return remote(
            here, here, top_send.at[i, bit], recv.at[i, 0], (flip(top, 1 << bit) * per + low, c)
        )

    def differs(bit):
        return lax.rem(top, 2 << bit) == lax.rem(c, 2 << bit)

    def forward_copy(i, mask, stage):
        b = orders[(i // unit) % 2][stage]
        part = pan.at[slot(i, mask)]
        return remote(
            part, part, send.at[i, mask, stage], recv.at[i, mask ^ (1 << b)],
            (flip(r, 1 << b), c),
        )

    def arrival(i, mask):
        part = pan.at[slot(i, mask)]
        return remote(part, part, chip_send, recv.at[i, mask], (r, c))

    def stages(position):
        return range(position.bit_length(), bits)

    for step, position in enumerate(positions):
        for i in range(ncol):
            mask = mask_of(i, position)
            if position == 0:

                @pl.when(jnp.logical_and(c == i, top == c))
                def _():
                    pltpu.make_async_copy(item_ref, pan.at[low * ncol + i], local_sem).wait()

                @pl.when(jnp.logical_not(jnp.logical_and(c == i, top == c)))
                def _():
                    arrival(i, 0).wait_recv()

                for bit in reversed(range(tops)):

                    @pl.when(differs(bit))
                    def _():
                        top_copy(i, bit).start()
            else:
                arrival(i, mask).wait_recv()
            for stage in stages(position):
                forward_copy(i, mask, stage).start()
        if position == 0:
            loop(1, ncol, lambda k: pair_arrival(k).wait_recv())
            for j in range(ncol):
                high, rest = split(pairs[j])
                ah[j * blk : (j + 1) * blk] = high
                al[j * blk : (j + 1) * blk] = rest
        buffer = step % 2
        for i in range(ncol):
            high, rest = split(pan[slot(i, mask_of(i, position)), :blk])
            at = slice((i % unit) * blk, (i % unit + 1) * blk)
            ph[i // unit, at] = high
            plo[i // unit, at] = rest
        for u in range(units):
            for copy in fetch(u, step, buffer):
                copy.wait()
        rows = min(256, points)
        width = min(blk, bands)

        for u in range(units):
            p2 = (ph[u], plo[u])
            lines = [
                pan[slot(i, mask_of(i, position)), blk : blk + EXTRA][j : j + 1, :width]
                for i in range(u * unit, (u + 1) * unit)
                for j in range(blk // width)
            ]

            def body(m):
                at = pl.ds(pl.multiple_of(m * rows, rows), rows)
                terms = dot3((ah[at], al[at]), p2, ((1,), (1,))) * wbuf[buffer, u, at]
                s_ref[at, :bands] += dot3(split(terms), p2, ((1,), (0,)))
                total = jnp.zeros((rows, 1), F32)
                for j, line in enumerate(lines):
                    part = bbuf[buffer, u, at, j * width : (j + 1) * width] * line
                    total = total + jnp.sum(part, axis=1, keepdims=True)
                s_ref[at, bands:] += jnp.broadcast_to(total, (rows, LANES))

            loop(0, points // rows, body)
        if step + 2 < per:
            start_fetch(step + 2)

    loop(1, ncol, lambda k: pair_copy(k).wait_send())

    @pl.when(top != c)
    def _():
        remote(item_ref, pan.at[low * ncol], chip_send, recv.at[0, 0], (r, top)).wait_send()

    for i in range(ncol):
        for bit in range(tops):

            @pl.when(differs(bit))
            def _():
                top_copy(i, bit).wait_send()

        for position in positions:
            for stage in stages(position):
                forward_copy(i, mask_of(i, position), stage).wait_send()


def last_kernel(
    nrow, ncol, size, s_ref, pv_ref, pc_ref, x_ref, prev_ref, gap_ref, beta_ref, out_ref, coef_ref,
    sin, kbuf, kin, rbuf, rin, tile1, tin1, tile2, tin2,
    s_send, s_recv, k_send, k_recv, r_send, r_recv, t1_send, t1_recv, t2_send, t2_recv,
):
    r, c = lax.axis_index("row"), lax.axis_index("col")
    blk, bands = pv_ref.shape
    h, w = x_ref.shape
    everyone = nrow * ncol
    me = r * ncol + c

    def col_peer(k):
        return lax.rem(c + k, ncol)

    def row_peer(k):
        return lax.rem(r + k, nrow)

    def s_copy(k):
        at = pl.ds(pl.multiple_of(col_peer(k) * blk, blk), blk)
        return remote(s_ref.at[at], sin.at[k], s_send.at[k], s_recv.at[k], (r, col_peer(k)))

    def k_copy(k):
        return remote(kbuf.at[col_peer(k)], kin.at[k], k_send.at[k], k_recv.at[k], (r, col_peer(k)))

    def r_copy(k):
        return remote(rbuf.at[row_peer(k)], rin.at[k], r_send.at[k], r_recv.at[k], (row_peer(k), c))

    loop(1, ncol, lambda k: s_copy(k).start())
    own = s_ref[pl.ds(pl.multiple_of(c * blk, blk), blk)]
    for k in range(1, ncol):
        s_copy(k).wait_recv()
        own = own + sin[k]
    terms = 2.0 * pv_ref[...] * own[:, bands : bands + 1] - own[:, :bands]
    turned = split(jnp.transpose(terms))
    for j in range(ncol):
        kbuf[j] = dot3(turned, split(pc_ref[:, j * w : (j + 1) * w]), ((1,), (0,)))
    loop(1, ncol, lambda k: k_copy(k).start())
    part = kbuf[c]
    for k in range(1, ncol):
        k_copy(k).wait_recv()
        part = part + kin[k]
    rbuf[...] = part.reshape(nrow, h, w)
    loop(1, nrow, lambda k: r_copy(k).start())
    x = x_ref[...]
    image = gap_ref[...] * x + rbuf[r]
    for k in range(1, nrow):
        r_copy(k).wait_recv()
        image = image + rin[k]

    def whole(a):
        return jnp.sum(jnp.sum(a, axis=0, keepdims=True), axis=1, keepdims=True)

    def shared(value, tile, tin, sends, recvs):
        def copy(k):
            there = lax.rem(me + k, everyone)
            return remote(tile, tin.at[me], sends.at[k], recvs.at[k], (there // ncol, lax.rem(there, ncol)))

        def arrival(k):
            there = lax.rem(me + everyone - k, everyone)
            return remote(tile, tin.at[there], sends.at[k], recvs.at[k], (there // ncol, lax.rem(there, ncol)))

        tile[...] = value
        tin[me] = value
        loop(1, everyone, lambda k: copy(k).start())
        loop(1, everyone, lambda k: arrival(k).wait_recv())
        loop(1, everyone, lambda k: copy(k).wait_send())
        return jnp.sum(tin[...], axis=0)

    line = lax.broadcasted_iota(jnp.int32, (8, LANES), 0)
    lane = lax.broadcasted_iota(jnp.int32, (1, LANES), 1)
    sums = shared(jnp.where(lane == 0, whole(x * image), whole(x * x)), tile1, tin1, t1_send, t1_recv)
    alpha = (sums[0:1, 0:1] / size) / (sums[0:1, 1:2] / size + epsilon)
    resid = image - alpha * x - beta_ref[...] * prev_ref[...]
    square = jnp.broadcast_to(whole(resid * resid), (1, LANES))
    beta = jnp.sqrt(shared(square, tile2, tin2, t2_send, t2_recv)[0:1, 0:1] / size + epsilon)
    out_ref[...] = resid / beta
    coef_ref[...] = jnp.where(line == 0, alpha, beta)
    loop(1, ncol, lambda k: s_copy(k).wait_send())
    loop(1, ncol, lambda k: k_copy(k).wait_send())
    loop(1, nrow, lambda k: r_copy(k).wait_send())


VM = pl.BlockSpec(memory_space=pltpu.VMEM)
DMA = pltpu.SemaphoreType.DMA
PARAMS = pltpu.CompilerParams(has_side_effects=True, vmem_limit_bytes=56 * 1024 * 1024)


def per_device(
    nrow, ncol, lanczos_now, lanczos_prev, beta_prev, valence_energy, conduction_energy,
    valence_panel, conduction_panel, screened_coulomb, bare_coulomb,
):
    chains, h, w = lanczos_now.shape
    blk, bands = valence_panel.shape
    conduction = conduction_panel.shape[1]
    points = screened_coulomb.shape[0]
    outs = []
    for chain in range(chains):
        x = lanczos_now[chain]
        full = pl.pallas_call(
            functools.partial(vectors_kernel, nrow, ncol),
            out_shape=jax.ShapeDtypeStruct((ncol, bands, w), F32),
            in_specs=[VM],
            out_specs=VM,
            scratch_shapes=[DMA(()), DMA((nrow,)), DMA((nrow,)), DMA((ncol,)), DMA((ncol,))],
            compiler_params=PARAMS,
        )(x)
        vectors = jnp.transpose(full, (1, 0, 2)).reshape(bands, conduction)
        pair = lax.dot_general(
            conduction_panel, vectors, (((1,), (1,)), ((), ())), precision=lax.Precision.HIGH,
            preferred_element_type=F32,
        )
        density = jnp.sum(pair * valence_panel, axis=1)
        width = min(blk, bands)
        lines = density.reshape(blk // width, width)
        lines = jnp.pad(lines, ((0, EXTRA - blk // width), (0, bands - width)))
        item = jnp.concatenate([valence_panel, lines], axis=0)
        unit = max(1, LANES // blk)
        per = nrow // ncol
        stages = max(1, per.bit_length() - 1)
        tops = max(1, ncol.bit_length() - 1)
        screened = pl.pallas_call(
            functools.partial(kernel_kernel, nrow, ncol, blk),
            out_shape=jax.ShapeDtypeStruct((points, bands + LANES), F32),
            in_specs=[VM, VM, pl.BlockSpec(memory_space=pl.ANY), pl.BlockSpec(memory_space=pl.ANY)],
            out_specs=VM,
            scratch_shapes=[
                pltpu.VMEM((nrow, blk + EXTRA, bands), F32),
                pltpu.VMEM((ncol, blk, bands), F32),
                pltpu.VMEM((points, bands), BF16),
                pltpu.VMEM((points, bands), BF16),
                pltpu.VMEM((ncol // unit, unit * blk, bands), BF16),
                pltpu.VMEM((ncol // unit, unit * blk, bands), BF16),
                pltpu.VMEM((2, ncol // unit, points, unit * blk), F32),
                pltpu.VMEM((2, ncol // unit, points, unit * blk), F32),
                DMA((2, ncol)),
                DMA((2, ncol)),
                DMA(()),
                DMA(()),
                DMA((ncol, tops)),
                DMA((ncol, per, stages)),
                DMA((ncol, per)),
                DMA((ncol,)),
                DMA((ncol,)),
            ],
            compiler_params=PARAMS,
        )(item, pair, screened_coulomb, bare_coulomb)
        gaps = conduction_energy[None, :] - valence_energy[:, None]
        beta = jnp.broadcast_to(beta_prev[chain], (1, w))
        everyone = nrow * ncol
        out, coef = pl.pallas_call(
            functools.partial(last_kernel, nrow, ncol, float(bands * conduction)),
            out_shape=(jax.ShapeDtypeStruct((h, w), F32), jax.ShapeDtypeStruct((8, LANES), F32)),
            in_specs=[VM] * 7,
            out_specs=(VM, VM),
            scratch_shapes=[
                pltpu.VMEM((ncol, blk, bands + LANES), F32),
                pltpu.VMEM((ncol, bands, w), F32),
                pltpu.VMEM((ncol, bands, w), F32),
                pltpu.VMEM((nrow, h, w), F32),
                pltpu.VMEM((nrow, h, w), F32),
                pltpu.VMEM((1, LANES), F32),
                pltpu.VMEM((everyone, 1, LANES), F32),
                pltpu.VMEM((1, LANES), F32),
                pltpu.VMEM((everyone, 1, LANES), F32),
            ]
            + [DMA((n,)) for n in (ncol, ncol, ncol, ncol, nrow, nrow) for _ in range(1)]
            + [DMA((everyone,))] * 4,
            compiler_params=PARAMS,
        )(screened, valence_panel, conduction_panel, x, lanczos_prev[chain], gaps, beta)
        outs.append((out, coef[:2, 0]))
    return jnp.stack([o for o, _ in outs]), jnp.stack([k for _, k in outs])


def solution(mesh):
    placed = (
        P(None, "row", "col"),
        P(None, "row", "col"),
        P(),
        P("row"),
        P("col"),
        P(("row", "col"), None),
        P(("row", "col"), None),
        P("row", "col"),
        P("row", "col"),
    )
    return jax.shard_map(
        functools.partial(per_device, mesh.shape["row"], mesh.shape["col"]),
        mesh=mesh,
        in_specs=placed,
        out_specs=(P(None, "row", "col"), P()),
        check_vma=False,
    )
```
